32 devices in a mesh: lat: 8 (over z, y), lon: 4 (over x, core).
Axes of the slice: x: 2, y: 2, z: 4, core: 2. Of those that a mesh axis runs over, the one named last changes fastest.
Arguments:
- raw_fields: bfloat16 [32, 160, 1440], P(('lat', 'lon')), may hold values from -6 to 6
- embed_weight: bfloat16 [32, 4, 4, 1024], replicated, may hold values from -0.25 to 0.25
- embed_bias: float32 [1024], replicated, may hold values from -3 to 3
- conv_weight: bfloat16 [3, 3, 1024, 1024], replicated, may hold values from -0.0625 to 0.0625
- conv_bias: float32 [1024], replicated, may hold values from -3 to 3
Outputs:
- features: bfloat16 [40, 360, 1024], P('lat', 'lon')
The draws below stay inside these ranges and needn't reach their ends.
All inputs are finite; a program needn't handle non-finite values.
Results may differ from the reference program's by a relative error of at most 0.0049.
Values may be sent and summed in bfloat16 or wider, within the bound.
A program may use at most 192 MiB of HBM per device.

```python
import jax
import jax.numpy as jnp

PATCH = 4
WIDTH = 1024
VARS = 32
HEIGHT = 160
BREADTH = 1440


def shard_levels(key, extent, split, least, top_value):
    level = 1.0
    for dim, shards_of in split:
        heights = jax.random.uniform(jax.random.fold_in(jax.random.fold_in(key, 6), dim), (shards_of,), jnp.float32, least / len(split), top_value / len(split))
        level = level * jnp.repeat(jnp.exp(heights), extent[dim] // shards_of).reshape((-1,) + (1,) * (len(extent) - 1 - dim))
    return level


def gaussian(own_key, dims, scale, most, pieces=(), kind=jnp.bfloat16):
    gain = shard_levels(own_key, dims, pieces, -0.22, 0.18) if pieces else 1.0
    values = jax.random.normal(own_key, dims, jnp.float32) * scale * gain
    return jnp.minimum(jnp.maximum(values, -most), most).astype(kind)


def setup_inputs(seed: int = 0) -> dict:
    arg_keys = jax.random.split(jax.random.key(seed), 6)
    return {
        "raw_fields": gaussian(arg_keys[0], (VARS, HEIGHT, BREADTH), 1.0, 6.0, ((0, 32),)),
        "embed_weight": gaussian(arg_keys[1], (VARS, PATCH, PATCH, WIDTH), (VARS * PATCH * PATCH) ** -0.5, 0.25),
        "embed_bias": gaussian(arg_keys[2], (WIDTH,), 0.5, 3.0, (), jnp.float32),
        "conv_weight": gaussian(arg_keys[3], (3, 3, WIDTH, WIDTH), (9 * WIDTH) ** -0.5, 0.0625),
        "conv_bias": gaussian(arg_keys[4], (WIDTH,), 0.5, 3.0, (), jnp.float32),
    }


def reference(raw_fields, embed_weight, embed_bias, conv_weight, conv_bias):
    count, height, breadth = raw_fields.shape
    patch_rows = height // PATCH
    patch_cols = breadth // PATCH
    grid_blocks = raw_fields.astype(jnp.float32).reshape(count, patch_rows, PATCH, patch_cols, PATCH)
    embedded = jnp.einsum("vaibj,vijd->abd", grid_blocks, embed_weight.astype(jnp.float32))
    embedded = (embedded + embed_bias).astype(jnp.bfloat16)
    channels = embedded.shape[2]
    padded = jnp.pad(embedded, ((0, 0), (1, 1), (0, 0)), mode="wrap")
    padded = jnp.pad(padded, ((1, 1), (0, 0), (0, 0)))
    summed = jnp.zeros((patch_rows * patch_cols, channels), jnp.float32)
    for step_row in range(3):
        for step_col in range(3):
            window = padded[step_row:step_row + patch_rows, step_col:step_col + patch_cols].reshape(-1, channels)
            summed = summed + jnp.dot(window, conv_weight[step_row, step_col], preferred_element_type=jnp.float32)
    summed = summed + conv_bias
    result = jax.nn.gelu(summed, approximate=False).astype(jnp.bfloat16)
    return result.reshape(patch_rows, patch_cols, channels)
```

```python
import functools

import jax
import jax.numpy as jnp
from jax import lax
from jax.experimental import pallas as pl
from jax.experimental.pallas import tpu as pltpu
from jax.sharding import PartitionSpec as P

PATCH = 4
LANES = 128
CELLS = PATCH * PATCH
MESH = pl.DeviceIdType.MESH
STEP = 256
WINDOW = 8


def kernel(
    dims,
    raw_hbm, ew_hbm, eb_hbm, cw_hbm, cb_hbm,
    out_ref,
    eb_ref, cb_ref, raw, sides, send, send_far, recv, recv_far, near, ew_raw, ew, cw, comb, bias, taps, acc,
    eb_sem, cb_sem, raw_sem, ew_sem, cw_sem, send_sem, fsend_sem, nsend_sem,
    edge_sem, rest_sem, far_sem, near_sem,
):
    lat_n, lon_n, height, breadth, rows, cols, width = dims
    total = lat_n * lon_n
    half_n = lat_n // 2
    lat = lax.axis_index("lat")
    lon = lax.axis_index("lon")
    me = lat * lon_n + lon
    mine = lat // half_n
    odd = lat % 2
    inside = (lat > 0) & (lat < lat_n - 1)
    row_slots = taps.shape[1] // (rows + 2)
    composed = total * CELLS <= width
    tap_width = total * CELLS if composed else width
    spare = LANES - row_slots
    tail = row_slots - LANES // 2
    tiles_n = rows - 1
    last = (tiles_n - 1) * LANES
    unrolled = total <= 32

    raw_copy = pltpu.make_async_copy(raw_hbm.at[0], raw, raw_sem)
    raw_copy.start()

    def peers(other, body):
        @pl.loop(1 - other, half_n * lon_n, unroll=unrolled)
        def _(step):
            k = step // lon_n
            base = (mine + other) % 2 * half_n
            local = (k // 2 * 2 + (k + lat) % 2) if other else (lat + k) % half_n
            body(base + local, (lon + step) % lon_n)

    barrier = pltpu.get_barrier_semaphore()

    def greet(a, b):
        pl.semaphore_signal(barrier, inc=1, device_id=(a, b), device_id_type=MESH)

    peers(1, greet)
    peers(0, greet)

    ew_copy = pltpu.make_async_copy(ew_hbm, ew_raw, ew_sem)
    ew_copy.start()
    bias_copies = [
        pltpu.make_async_copy(eb_hbm, eb_ref, eb_sem),
        pltpu.make_async_copy(cb_hbm, cb_ref, cb_sem),
    ]
    for copy in bias_copies:
        copy.start()

    unit_n = width // 2
    units = 18

    def fetch(unit):
        p, q, n = unit // 6, unit // 2 % 3, pl.multiple_of(unit % 2 * unit_n, unit_n)
        return pltpu.make_async_copy(
            cw_hbm.at[p, q, :, pl.ds(n, unit_n)], cw.at[p, q, :, pl.ds(n, unit_n)], cw_sem.at[unit]
        )

    patches = breadth // PATCH
    group = min(lat_n, 8)
    group_rows = group * rows * PATCH
    block = group * CELLS
    lane = lax.broadcasted_iota(jnp.int32, (1, PATCH * LANES), 1)
    slot = lane % LANES
    cell = lane // LANES
    m = lax.broadcasted_iota(jnp.int32, (rows * block, 1), 0)
    target = (
        (m % PATCH) * group_rows
        + ((m // CELLS) % group) * (rows * PATCH)
        + (m // block) * PATCH
        + (m // PATCH) % PATCH
    )
    c = lax.broadcasted_iota(jnp.int32, (rows * block, PATCH * group_rows), 1)
    pick_rows = jnp.where(c == target, 1.0, 0.0).astype(jnp.bfloat16)
    pickers = []
    for l in range(lon_n):
        wanted = [PATCH * ((cols * l - 1 + s) % patches) for s in range(cols + 2)]
        used = sorted({x // LANES for w in wanted for x in (w, w + PATCH - 1)})
        patch = (cols * l - 1 + slot + patches) % patches
        column = jnp.where(slot < cols + 2, PATCH * patch + cell, -1)
        picks = []
        for b in used:
            k = lax.broadcasted_iota(jnp.int32, (LANES, PATCH * LANES), 0) + b * LANES
            picks.append(jnp.where(k == column, 1.0, 0.0).astype(jnp.bfloat16))
        pickers.append((used, jnp.concatenate(picks, axis=0)))

    @pl.when(jnp.logical_not(inside))
    def _():
        recv_far[...] = jnp.zeros(recv_far.shape, jnp.bfloat16)

    for unit in range(WINDOW // 2):
        fetch(unit).start()
    raw_copy.wait()
    left_half = lax.broadcasted_iota(jnp.int32, (CELLS // 2, LANES), 1) < LANES // 2
    for g in range(lat_n // group):
        for l in range(lon_n):
            used, picks = pickers[l]
            parts = []
            for b in used:
                part = raw[
                    g * group_rows : (g + 1) * group_rows,
                    b * LANES : min((b + 1) * LANES, breadth),
                ]
                short = LANES - part.shape[1]
                if short:
                    fill = jnp.zeros((group_rows, short), jnp.bfloat16)
                    part = jnp.concatenate([part, fill], axis=1)
                parts.append(part)
            found = jnp.dot(
                jnp.concatenate(parts, axis=1), picks, preferred_element_type=jnp.float32
            ).astype(jnp.bfloat16)
            for j in range(PATCH):
                sides[j * group_rows : (j + 1) * group_rows, l * LANES : (l + 1) * LANES] = (
                    found[:, j * LANES : (j + 1) * LANES]
                )
        tiles = jnp.dot(pick_rows, sides[...], preferred_element_type=jnp.float32)
        low = lax.broadcasted_iota(jnp.int32, (block, LANES), 1) < row_slots
        for l in range(lon_n):
            column = tiles[:, l * LANES : (l + 1) * LANES]
            per_row = [column[a * block : (a + 1) * block] for a in range(rows)]
            spread = per_row[rows - 2]
            here = slice(g * group, (g + 1) * group)
            for k in range(tiles_n):
                kept = per_row[k if k < rows - 2 else rows - 1]
                if k < tiles_n - 1:
                    if k * spare < row_slots:
                        kept = jnp.where(low, kept, pltpu.roll(spread, row_slots - k * spare, 1))
                    send[here, l, :, k * LANES : (k + 1) * LANES] = (
                        kept.astype(jnp.bfloat16).reshape(group, CELLS, LANES)
                    )
                else:
                    send[here, l, :, last : last + row_slots] = (
                        kept.astype(jnp.bfloat16).reshape(group, CELLS, LANES)[:, :, :row_slots]
                    )
            for t in range(group):
                at = g * group + t
                to = at + 1 if t % 2 else at - 1
                if 0 <= to < lat_n:
                    far = per_row[rows - 1 if t % 2 else 0][t * CELLS : (t + 1) * CELLS]
                    ends = pltpu.roll(far, spare, 1).astype(jnp.bfloat16)
                    send[to, l, :, last + row_slots : last + LANES] = ends[:, row_slots:]
                    folded = jnp.where(
                        left_half, far[: CELLS // 2], pltpu.roll(far[CELLS // 2 :], LANES // 2, 1)
                    )
                    send_far[to, l] = folded.astype(jnp.bfloat16)
                if at in (0, lat_n - 1):
                    send[at, l, :, last + row_slots : last + LANES] = jnp.zeros(
                        (CELLS, spare), jnp.bfloat16
                    )

    for unit in range(WINDOW // 2, WINDOW):
        fetch(unit).start()

    ew_copy.wait()
    for copy in bias_copies:
        copy.wait()
    for i in range(PATCH):
        ew[:total, PATCH * i : PATCH * (i + 1), :] = ew_raw[:, i]
    if composed:
        high = eb_ref[...].astype(jnp.bfloat16)
        rest = eb_ref[...] - high.astype(jnp.float32)
        index = lax.broadcasted_iota(jnp.int32, (CELLS, width), 0)
        both = jnp.where(index == 0, high.astype(jnp.float32), jnp.where(index == 1, rest, 0.0))
        ew[total] = both.astype(jnp.bfloat16)

    def compose(start, stop):
        @pl.loop(start, stop)
        def _(unit):
            p, q = unit // 6, unit // 2 % 3
            fetch(unit).wait()

            @pl.when(unit + WINDOW < units)
            def _():
                fetch(unit + WINDOW).start()

            if composed:
                left = ew[...].reshape((total + 1) * CELLS, width)
                for step in range(0, unit_n, STEP):
                    n = pl.multiple_of(unit % 2 * unit_n + step, STEP)
                    product = jnp.dot(
                        left, cw[p, q, :, pl.ds(n, STEP)], preferred_element_type=jnp.float32
                    )
                    comb[p, q, :, pl.ds(n, STEP)] = product[:tap_width].astype(jnp.bfloat16)
                    bias[3 * p + q, :, pl.ds(n, STEP)] = product[tap_width : tap_width + 8]

    hops = lat // 2 + odd + lon // 2
    early = (8 + hops) // (1 + hops * hops)
    compose(0, early)

    pl.semaphore_wait(barrier, total - 1)

    def edge_tile(parity):
        return pl.multiple_of((1 - parity) * last, LANES)

    def rest_tiles(parity):
        return pl.multiple_of(parity * LANES, LANES)

    def remote(source, dest, out_sem, in_sem, a, b):
        pltpu.make_async_remote_copy(
            src_ref=source, dst_ref=dest, send_sem=out_sem, recv_sem=in_sem,
            device_id=(a, b), device_id_type=MESH,
        ).start()

    def exchange(part, other):
        def body(a, b):
            if part == "edge":
                at = pl.ds(edge_tile(a % 2), LANES)
                remote(send.at[a, b, :, at], recv.at[me, :, at], send_sem, edge_sem.at[other], a, b)
            if part == "rest":
                at = pl.ds(rest_tiles(a % 2), last)
                remote(send.at[a, b, :, at], recv.at[me, :, at], send_sem, rest_sem.at[other], a, b)
            if part == "far":
                @pl.when((a > 0) & (a < lat_n - 1))
                def _():
                    remote(send_far.at[a, b], recv_far.at[me], fsend_sem, far_sem.at[other], a, b)

        peers(other, body)

    exchange("edge", 1)
    exchange("edge", 0)
    at = pl.ds(edge_tile(odd), LANES)
    pltpu.make_async_copy(send.at[lat, lon, :, at], recv.at[me, :, at], edge_sem.at[0]).start()
    at = pl.ds(rest_tiles(odd), last)
    pltpu.make_async_copy(send.at[lat, lon, :, at], recv.at[me, :, at], rest_sem.at[0]).start()

    @pl.when(inside)
    def _():
        pltpu.make_async_copy(send_far.at[lat, lon], recv_far.at[me], far_sem.at[0]).start()

    exchange("rest", 0)
    exchange("far", 0)
    exchange("rest", 1)
    exchange("far", 1)

    count = half_n * lon_n

    def sources(other):
        return pl.ds(pl.multiple_of((mine + other) % 2 * count, count), count)

    def near_copy(other):
        return pltpu.make_async_remote_copy(
            src_ref=recv.at[sources(other), :, pl.ds(edge_tile(odd), LANES)],
            dst_ref=near.at[sources(other)],
            send_sem=nsend_sem.at[other],
            recv_sem=near_sem.at[other],
            device_id=(lat + 1 - 2 * odd, lon),
            device_id_type=MESH,
        )

    def arrived(ref, sem):
        pltpu.make_async_copy(ref, ref, sem).wait()

    def forward_near(other):
        arrived(recv.at[sources(other), :, pl.ds(0, LANES)], edge_sem.at[other])
        near_copy(other).start()

    def wait_rest(other):
        arrived(recv.at[sources(other), :, pl.ds(0, last)], rest_sem.at[other])

    def wait_far(other):
        @pl.when(inside)
        def _():
            arrived(recv_far.at[sources(other)], far_sem.at[other])

    compose(early, 11)
    forward_near(0)
    compose(11, 15)
    forward_near(1)
    compose(15, units)

    groups = 2 if composed else 1
    group_width = tap_width // groups
    kernel_weights = comb if composed else cw

    def taken(ref, g):
        return ref[sources(g)] if composed else ref[...]

    def place(g, row, n, tokens):
        lanes = slice(n, n + tokens.shape[1])
        start = row * row_slots
        if not isinstance(start, int):
            start = pl.multiple_of(start, 16)
        for q in range(3):
            shifted = tokens if q == 0 else pltpu.roll(tokens, row_slots - q, 0)
            lo = q * group_width
            taps[g, pl.ds(start, row_slots), lo + lanes.start : lo + lanes.stop] = (
                shifted.astype(jnp.bfloat16)
            )

    def embed(x, n):
        if composed:
            return x[:, n : n + STEP].astype(jnp.float32)
        weights = ew[:total, :, n : n + STEP].reshape(total * CELLS, STEP)
        return jnp.dot(x, weights, preferred_element_type=jnp.float32) + eb_ref[:, n : n + STEP]

    def flat(x):
        return x.reshape(x.shape[0] * CELLS, x.shape[2]).T

    def place_rest(g):
        x = flat(taken(recv, g))
        for n in range(0, group_width, STEP):
            e = embed(x, n)
            chunks = []
            for k in range(tiles_n):
                row = k if k < rows - 2 else rows - 1
                place(g, row + 1, n, e[k * LANES : k * LANES + row_slots])
                if k * spare < row_slots:
                    chunks.append(e[k * LANES + row_slots : (k + 1) * LANES])
            place(g, rows - 1, n, jnp.concatenate(chunks, axis=0)[:row_slots])

    def place_near(g):
        x = flat(taken(near, g))[:row_slots]
        for n in range(0, group_width, STEP):
            place(g, (rows + 1) * (1 - odd), n, embed(x, n))

    def place_far(g):
        folded = taken(recv_far, g).astype(jnp.float32)
        n_src = folded.shape[0]
        turned = pltpu.roll(folded.reshape(n_src * CELLS // 2, LANES), LANES // 2, 1)
        whole = jnp.concatenate([folded, turned.reshape(folded.shape)], axis=1)
        x = flat(whole)[: LANES // 2].astype(jnp.bfloat16)
        edge = recv[sources(g), :, last:] if composed else recv[:, :, last:]
        ends = flat(edge)[row_slots : row_slots + tail]
        x = jnp.concatenate([x, ends], axis=0)
        for n in range(0, group_width, STEP):
            e = embed(x, n)
            if not composed:
                e = e * jnp.where(inside, 1.0, 0.0)
            place(g, (rows + 1) * odd, n, e)

    top = jnp.where(lat > 0, 1.0, 0.0)
    bottom = jnp.where(lat < lat_n - 1, 1.0, 0.0)

    def row_bias(n, scales):
        total_bias = cb_ref[:, pl.ds(n, STEP)]
        if composed:
            for p in range(3):
                part = 0.0
                for q in range(3):
                    part += bias[3 * p + q, 0:1, pl.ds(n, STEP)] + bias[3 * p + q, 1:2, pl.ds(n, STEP)]
                total_bias = total_bias + part * scales[p]
        return total_bias

    def rows_at(a, n_rows):
        return pl.ds(pl.multiple_of(a * row_slots, 16), n_rows * row_slots)

    def conv(g, a, n_rows, first, final):
        @pl.loop(0, width // (2 * STEP))
        def _(block_n):
            for part_n in range(2):
                n = pl.multiple_of(block_n * (2 * STEP) + part_n * STEP, STEP)
                at_n = pl.ds(n, STEP)
                summed = None
                for p in range(3):
                    if composed:
                        chosen = pl.ds(pl.multiple_of((mine + g) % 2 * group_width, group_width), group_width)
                        weights = kernel_weights[p, :, chosen, at_n]
                    else:
                        weights = kernel_weights[p, :, :, at_n]
                    part = jnp.dot(
                        taps[g, rows_at(a + p, n_rows), :],
                        weights.reshape(3 * group_width, STEP),
                        preferred_element_type=jnp.float32,
                    )
                    summed = part if summed is None else summed + part
                if first:
                    shift = row_bias(n, (1.0, 1.0, 1.0))
                    above, below = row_bias(n, (top, 1.0, 1.0)), row_bias(n, (1.0, 1.0, bottom))
                for k in range(n_rows):
                    value = summed[k * row_slots : (k + 1) * row_slots]
                    if first:
                        value = value + (above if k == 0 else below if k == rows - 1 else shift)
                    else:
                        value = value + acc[rows_at(a + k, 1), at_n]
                    if final:
                        value = 0.5 * value * (1.0 + lax.erf(value * (0.5 ** 0.5)))
                        out_ref[a + k, :, at_n] = value[:cols].astype(jnp.bfloat16)
                    else:
                        acc[rows_at(a + k, 1), at_n] = value

    main_row, far_row = 1 - odd, (rows - 1) * odd
    if composed:
        wait_rest(0)
        place_rest(0)
        near_copy(0).wait_recv()
        place_near(0)
        wait_far(0)
        place_far(0)
        conv(0, 0, rows, True, False)
        wait_rest(1)
        place_rest(1)
        near_copy(1).wait_recv()
        place_near(1)
        conv(1, main_row, rows - 1, False, True)
        wait_far(1)
        place_far(1)
        conv(1, far_row, 1, False, True)
    else:
        for other in range(2):
            wait_rest(other)
            near_copy(other).wait_recv()
            wait_far(other)
        place_rest(0)
        place_near(0)
        place_far(0)
        conv(0, 0, rows, True, True)

    sent = pl.ds(0, total - 1)
    arrived(recv.at[sent], send_sem)
    targets = (lat_n - 2) * lon_n

    @pl.when(inside)
    def _():
        arrived(recv_far.at[pl.ds(0, targets - 1)], fsend_sem)

    @pl.when(jnp.logical_not(inside))
    def _():
        arrived(recv_far.at[pl.ds(0, targets)], fsend_sem)

    near_copy(0).wait_send()
    near_copy(1).wait_send()


def per_device(raw_fields, embed_weight, embed_bias, conv_weight, conv_bias):
    lat_n = lax.axis_size("lat")
    lon_n = lax.axis_size("lon")
    total = lat_n * lon_n
    var_dev, height, breadth = raw_fields.shape
    assert var_dev == 1 and lat_n % 4 == 0
    rows = height // lat_n // PATCH
    cols = breadth // lon_n // PATCH
    width = embed_weight.shape[3]
    row_slots = (cols + 2 + 15) // 16 * 16
    spare = LANES - row_slots
    assert LANES // 2 < row_slots < LANES and spare * (rows - 2) >= row_slots
    assert row_slots - LANES // 2 <= spare
    dims = (lat_n, lon_n, height, breadth, rows, cols, width)
    group = min(lat_n, 8)
    bf16 = jnp.bfloat16
    composed = total * CELLS <= width
    tap_width = total * CELLS if composed else width
    groups = 2 if composed else 1
    any_space = pl.BlockSpec(memory_space=pltpu.HBM)
    vmem = pl.BlockSpec(memory_space=pltpu.VMEM)
    return pl.pallas_call(
        functools.partial(kernel, dims),
        out_shape=jax.ShapeDtypeStruct((rows, cols, width), bf16),
        in_specs=[any_space]*5,
        out_specs=vmem,
        scratch_shapes=[
            pltpu.VMEM((1, width), jnp.float32),
            pltpu.VMEM((1, width), jnp.float32),
            pltpu.VMEM((height, breadth), bf16),
            pltpu.VMEM((PATCH * group * rows * PATCH, lon_n * LANES), bf16),
            pltpu.VMEM((lat_n, lon_n, CELLS, (rows - 1) * LANES), bf16),
            pltpu.VMEM((lat_n, lon_n, CELLS // 2, LANES), bf16),
            pltpu.VMEM((total, CELLS, (rows - 1) * LANES), bf16),
            pltpu.VMEM((total, CELLS // 2, LANES), bf16),
            pltpu.VMEM((total, CELLS, LANES), bf16),
            pltpu.VMEM((total, PATCH, PATCH, width), bf16),
            pltpu.VMEM((total + 1, CELLS, width), bf16),
            pltpu.VMEM((3, 3, width, width), bf16),
            pltpu.VMEM((3, 3, tap_width if composed else CELLS, width), bf16),
            pltpu.VMEM((9, 8, width), jnp.float32),
            pltpu.VMEM((groups, (rows + 2) * row_slots, 3 * tap_width // groups), bf16),
            pltpu.VMEM((rows * row_slots, width if composed else LANES), jnp.float32),
            pltpu.SemaphoreType.DMA,
            pltpu.SemaphoreType.DMA,
            pltpu.SemaphoreType.DMA,
            pltpu.SemaphoreType.DMA,
            pltpu.SemaphoreType.DMA((18,)),
            pltpu.SemaphoreType.DMA,
            pltpu.SemaphoreType.DMA,
            pltpu.SemaphoreType.DMA((2,)),
            pltpu.SemaphoreType.DMA((2,)),
            pltpu.SemaphoreType.DMA((2,)),
            pltpu.SemaphoreType.DMA((2,)),
            pltpu.SemaphoreType.DMA((2,)),
        ],
        compiler_params=pltpu.CompilerParams(
            collective_id=0, has_side_effects=True, vmem_limit_bytes=50 * 1024 * 1024
        ),
        name="tiles",
    )(
        *(pltpu.with_memory_space_constraint(v, pltpu.HBM) for v in (raw_fields, embed_weight, embed_bias.reshape(1, width), conv_weight, conv_bias.reshape(1, width))),
    )


def solution(mesh):
    return jax.shard_map(
        per_device,
        mesh=mesh,
        in_specs=(P(("lat", "lon"), None, None), P(), P(), P(), P()),
        out_specs=P("lat", "lon", None),
        check_vma=False,
    )
```

```python
import functools

import jax
import jax.numpy as jnp
from jax import lax
from jax.experimental import pallas as pl
from jax.experimental.pallas import tpu as pltpu
from jax.sharding import PartitionSpec as P

PATCH = 4
LANES = 128
CELLS = PATCH * PATCH
MESH = pl.DeviceIdType.MESH
STEP = 256
WINDOW = 9
FIRST = 6


def kernel(
    dims,
    raw_hbm, ew_hbm, eb_hbm, cw_hbm, cb_hbm,
    out_ref,
    eb_ref, cb_ref, raw, sides, send, send_far, far_ends, recv, recv_far, near, ew_raw, ew, cw, comb, bias, taps, acc,
    eb_sem, cb_sem, raw_sem, ew_sem, cw_sem, send_sem, fsend_sem, nsend_sem,
    edge_sem, rest_sem, far_sem, near_sem,
):
    lat_n, lon_n, height, breadth, rows, cols, width = dims
    total = lat_n * lon_n
    half_n = lat_n // 2
    lat = lax.axis_index("lat")
    lon = lax.axis_index("lon")
    me = lat * lon_n + lon
    mine = lat // half_n
    odd = lat % 2
    inside = (lat > 0) & (lat < lat_n - 1)
    row_slots = taps.shape[1] // (rows + 2)
    composed = total * CELLS <= width
    tap_width = total * CELLS if composed else width
    spare = LANES - row_slots
    tail = row_slots - LANES // 2
    tiles_n = rows - 1
    last = (tiles_n - 1) * LANES
    unrolled = total <= 32

    raw_copy = pltpu.make_async_copy(raw_hbm.at[0], raw, raw_sem)
    raw_copy.start()

    def peers(other, body):
        @pl.loop(1 - other, half_n * lon_n, unroll=unrolled)
        def _(step):
            k = step // lon_n
            base = (mine + other) % 2 * half_n
            local = (k // 2 * 2 + (k + lat) % 2) if other else (lat + k) % half_n
            body(base + local, (lon + step) % lon_n)

    barrier = pltpu.get_barrier_semaphore()

    def greet(a, b):
        pl.semaphore_signal(barrier, inc=1, device_id=(a, b), device_id_type=MESH)

    peers(1, greet)
    peers(0, greet)

    ew_copy = pltpu.make_async_copy(ew_hbm, ew_raw, ew_sem)
    ew_copy.start()
    bias_copies = [
        pltpu.make_async_copy(eb_hbm, eb_ref, eb_sem),
        pltpu.make_async_copy(cb_hbm, cb_ref, cb_sem),
    ]
    for copy in bias_copies:
        copy.start()

    unit_n = width // 2
    units = 18

    def fetch(unit):
        p, q, n = unit // 6, unit // 2 % 3, pl.multiple_of(unit % 2 * unit_n, unit_n)
        return pltpu.make_async_copy(
            cw_hbm.at[p, q, :, pl.ds(n, unit_n)], cw.at[p, q, :, pl.ds(n, unit_n)], cw_sem.at[unit]
        )

    patches = breadth // PATCH
    group = min(lat_n, 8)
    group_rows = group * rows * PATCH
    block = group * CELLS
    lane = lax.broadcasted_iota(jnp.int32, (1, PATCH * LANES), 1)
    slot = lane % LANES
    cell = lane // LANES
    m = lax.broadcasted_iota(jnp.int32, (rows * block, 1), 0)
    target = (
        (m % PATCH) * group_rows
        + ((m // CELLS) % group) * (rows * PATCH)
        + (m // block) * PATCH
        + (m // PATCH) % PATCH
    )
    c = lax.broadcasted_iota(jnp.int32, (rows * block, PATCH * group_rows), 1)
    pick_rows = jnp.where(c == target, 1.0, 0.0).astype(jnp.bfloat16)
    pickers = []
    for l in range(lon_n):
        wanted = [PATCH * ((cols * l - 1 + s) % patches) for s in range(cols + 2)]
        used = sorted({x // LANES for w in wanted for x in (w, w + PATCH - 1)})
        patch = (cols * l - 1 + slot + patches) % patches
        column = jnp.where(slot < cols + 2, PATCH * patch + cell, -1)
        picks = []
        for b in used:
            k = lax.broadcasted_iota(jnp.int32, (LANES, PATCH * LANES), 0) + b * LANES
            picks.append(jnp.where(k == column, 1.0, 0.0).astype(jnp.bfloat16))
        pickers.append((used, jnp.concatenate(picks, axis=0)))

    @pl.when(jnp.logical_not(inside))
    def _():
        recv_far[...] = jnp.zeros(recv_far.shape, jnp.bfloat16)

    for unit in range(FIRST):
        fetch(unit).start()
    raw_copy.wait()
    left_half = lax.broadcasted_iota(jnp.int32, (CELLS // 2, LANES), 1) < LANES // 2
    for g in range(lat_n // group):
        for l in range(lon_n):
            used, picks = pickers[l]
            parts = []
            for b in used:
                part = raw[
                    g * group_rows : (g + 1) * group_rows,
                    b * LANES : min((b + 1) * LANES, breadth),
                ]
                short = LANES - part.shape[1]
                if short:
                    fill = jnp.zeros((group_rows, short), jnp.bfloat16)
                    part = jnp.concatenate([part, fill], axis=1)
                parts.append(part)
            found = jnp.dot(
                jnp.concatenate(parts, axis=1), picks, preferred_element_type=jnp.float32
            ).astype(jnp.bfloat16)
            for j in range(PATCH):
                sides[j * group_rows : (j + 1) * group_rows, l * LANES : (l + 1) * LANES] = (
                    found[:, j * LANES : (j + 1) * LANES]
                )
        tiles = jnp.dot(pick_rows, sides[...], preferred_element_type=jnp.float32)
        low = lax.broadcasted_iota(jnp.int32, (block, LANES), 1) < row_slots
        even = lax.broadcasted_iota(jnp.int32, (block, LANES), 0) // CELLS % 2 == 0
        for l in range(lon_n):
            column = tiles[:, l * LANES : (l + 1) * LANES]
            per_row = [column[a * block : (a + 1) * block] for a in range(rows)]
            spread = per_row[rows - 2]
            here = slice(g * group, (g + 1) * group)
            turned = [pltpu.roll(spread, row_slots - k * spare, 1) for k in range(tiles_n - 1)]
            for k in range(tiles_n):
                kept = per_row[k if k < rows - 2 else rows - 1]
                kept = jnp.where(
                    low, kept, jnp.where(even, turned[min(k, tiles_n - 2)], turned[max(k - 1, 0)])
                )
                send[here, l, :, k * LANES : (k + 1) * LANES] = (
                    kept.astype(jnp.bfloat16).reshape(group, CELLS, LANES)
                )
            for t in range(group):
                at = g * group + t
                to = at + 1 if t % 2 else at - 1
                if 0 <= to < lat_n:
                    far = per_row[rows - 1 if t % 2 else 0][t * CELLS : (t + 1) * CELLS]
                    ends = pltpu.roll(far, spare, 1).astype(jnp.bfloat16)
                    far_ends[to, l, :, row_slots:] = ends[:, row_slots:]
                    folded = jnp.where(
                        left_half, far[: CELLS // 2], pltpu.roll(far[CELLS // 2 :], LANES // 2, 1)
                    )
                    send_far[to, l] = folded.astype(jnp.bfloat16)
                if at in (0, lat_n - 1):
                    far_ends[at, l, :, row_slots:] = jnp.zeros((CELLS, spare), jnp.bfloat16)
    for t in range(lat_n):
        tile = 0 if t % 2 else last
        send[t, :, :, tile + row_slots : tile + LANES] = far_ends[t, :, :, row_slots:]

    for unit in range(FIRST, WINDOW):
        fetch(unit).start()

    ew_copy.wait()
    for copy in bias_copies:
        copy.wait()
    for i in range(PATCH):
        ew[:total, PATCH * i : PATCH * (i + 1), :] = ew_raw[:, i]
    if composed:
        high = eb_ref[...].astype(jnp.bfloat16)
        rest = eb_ref[...] - high.astype(jnp.float32)
        index = lax.broadcasted_iota(jnp.int32, (CELLS, width), 0)
        both = jnp.where(index == 0, high.astype(jnp.float32), jnp.where(index == 1, rest, 0.0))
        ew[total] = both.astype(jnp.bfloat16)

    def compose(start, stop):
        for unit in range(start, stop):
            fetch(unit).wait()
        for unit in range(start + WINDOW, min(stop + WINDOW, units)):
            fetch(unit).start()
        if composed:
            left = ew[...].reshape((total + 1) * CELLS, width)
            for unit in range(start, stop):
                p, q = unit // 6, unit // 2 % 3
                for step in range(0, unit_n, STEP):
                    n = unit % 2 * unit_n + step
                    product = jnp.dot(
                        left, cw[p, q, :, n : n + STEP], preferred_element_type=jnp.float32
                    )
                    comb[p, q, :, n : n + STEP] = product[:tap_width].astype(jnp.bfloat16)
                    bias[3 * p + q, :, n : n + STEP] = product[tap_width : tap_width + 8]

    def edge_tile(parity):
        return pl.multiple_of((1 - parity) * last, LANES)

    def rest_tiles(parity):
        return pl.multiple_of(parity * LANES, LANES)

    def remote(source, dest, out_sem, in_sem, a, b):
        pltpu.make_async_remote_copy(
            src_ref=source, dst_ref=dest, send_sem=out_sem, recv_sem=in_sem,
            device_id=(a, b), device_id_type=MESH,
        ).start()

    def exchange(part, other):
        def body(a, b):
            if part == "edge":
                at = pl.ds(edge_tile(a % 2), LANES)
                remote(send.at[a, b, :, at], recv.at[me, :, at], send_sem, edge_sem.at[other], a, b)
            if part == "near":
                at = pl.ds(edge_tile(1 - a % 2), LANES)
                source = send.at[a + 1 - 2 * (a % 2), b, :, at]
                remote(source, near.at[me], nsend_sem.at[0], near_sem.at[0], a, b)
            if part == "rest":
                at = pl.ds(rest_tiles(a % 2), last)
                remote(send.at[a, b, :, at], recv.at[me, :, at], send_sem, rest_sem.at[other], a, b)
            if part == "far":
                @pl.when((a > 0) & (a < lat_n - 1))
                def _():
                    remote(send_far.at[a, b], recv_far.at[me], fsend_sem, far_sem.at[other], a, b)

        peers(other, body)

    def issue():
        pl.semaphore_wait(barrier, total - 1)
        exchange("edge", 1)
        exchange("edge", 0)
        exchange("near", 0)
        exchange("far", 0)
        exchange("far", 1)
        exchange("rest", 0)
        exchange("rest", 1)
        own = pl.ds(edge_tile(odd), LANES)
        pltpu.make_async_copy(send.at[lat, lon, :, own], recv.at[me, :, own], edge_sem.at[0]).start()
        pair = pl.ds(edge_tile(1 - odd), LANES)
        pltpu.make_async_copy(
            send.at[lat + 1 - 2 * odd, lon, :, pair], near.at[me], near_sem.at[0]
        ).start()
        own = pl.ds(rest_tiles(odd), last)
        pltpu.make_async_copy(send.at[lat, lon, :, own], recv.at[me, :, own], rest_sem.at[0]).start()

        @pl.when(inside)
        def _():
            pltpu.make_async_copy(send_far.at[lat, lon], recv_far.at[me], far_sem.at[0]).start()

    count = half_n * lon_n

    def sources(other):
        return pl.ds(pl.multiple_of((mine + other) % 2 * count, count), count)

    def near_copy():
        return pltpu.make_async_remote_copy(
            src_ref=recv.at[sources(1), :, pl.ds(edge_tile(odd), LANES)],
            dst_ref=near.at[sources(1)],
            send_sem=nsend_sem.at[1],
            recv_sem=near_sem.at[1],
            device_id=(lat + 1 - 2 * odd, lon),
            device_id_type=MESH,
        )

    def arrived(ref, sem):
        pltpu.make_async_copy(ref, ref, sem).wait()

    def wait_edge(other):
        arrived(recv.at[sources(other), :, pl.ds(0, LANES)], edge_sem.at[other])

    def forward_near():
        wait_edge(1)
        near_copy().start()

    def wait_near(other):
        arrived(near.at[sources(other)], near_sem.at[other])

    def wait_rest(other):
        arrived(recv.at[sources(other), :, pl.ds(0, last)], rest_sem.at[other])

    def wait_far(other):
        @pl.when(inside)
        def _():
            arrived(recv_far.at[sources(other)], far_sem.at[other])

    hops = lat // 2 + odd + lon // 2
    early = (0, 2, 4, 8)
    for k, stop in enumerate(early):
        if k:
            compose(early[k - 1], stop)
        pl.when(jnp.maximum(len(early) - 1 - hops, 0) == k)(issue)
    compose(early[-1], 15)
    forward_near()
    compose(15, units)

    groups = 2 if composed else 1
    group_width = tap_width // groups
    kernel_weights = comb if composed else cw

    def taken(ref, g):
        return ref[sources(g)] if composed else ref[...]

    def place(g, row, n, tokens):
        lanes = slice(n, n + tokens.shape[1])
        start = row * row_slots
        if not isinstance(start, int):
            start = pl.multiple_of(start, 16)
        for q in range(3):
            shifted = tokens if q == 0 else pltpu.roll(tokens, row_slots - q, 0)
            lo = q * group_width
            taps[g, pl.ds(start, row_slots), lo + lanes.start : lo + lanes.stop] = (
                shifted.astype(jnp.bfloat16)
            )

    def embed(x, n):
        if composed:
            return x[:, n : n + STEP].astype(jnp.float32)
        weights = ew[:total, :, n : n + STEP].reshape(total * CELLS, STEP)
        return jnp.dot(x, weights, preferred_element_type=jnp.float32) + eb_ref[:, n : n + STEP]

    def flat(x):
        return x.reshape(x.shape[0] * CELLS, x.shape[2]).T

    def place_rest(g):
        x = flat(taken(recv, g))
        for n in range(0, group_width, STEP):
            e = embed(x, n)
            chunks = []
            for k in range(tiles_n):
                row = k if k < rows - 2 else rows - 1
                place(g, row + 1, n, e[k * LANES : k * LANES + row_slots])
                chunks.append(e[k * LANES + row_slots : (k + 1) * LANES])
            kept = [
                jnp.where(odd > 0, chunks[k + 1], chunks[k]) for k in range(tiles_n - 1)
            ]
            place(g, rows - 1, n, jnp.concatenate(kept, axis=0)[:row_slots])

    def place_near(g):
        x = flat(taken(near, g))[:row_slots]
        for n in range(0, group_width, STEP):
            place(g, (rows + 1) * (1 - odd), n, embed(x, n))

    def place_far(g):
        folded = taken(recv_far, g).astype(jnp.float32)
        n_src = folded.shape[0]
        turned = pltpu.roll(folded.reshape(n_src * CELLS // 2, LANES), LANES // 2, 1)
        whole = jnp.concatenate([folded, turned.reshape(folded.shape)], axis=1)
        x = flat(whole)[: LANES // 2].astype(jnp.bfloat16)
        at = pl.ds(edge_tile(odd), LANES)
        edge = recv[sources(g), :, at] if composed else recv[:, :, at]
        ends = flat(edge)[row_slots : row_slots + tail]
        x = jnp.concatenate([x, ends], axis=0)
        for n in range(0, group_width, STEP):
            e = embed(x, n)
            if not composed:
                e = e * jnp.where(inside, 1.0, 0.0)
            place(g, (rows + 1) * odd, n, e)

    top = jnp.where(lat > 0, 1.0, 0.0)
    bottom = jnp.where(lat < lat_n - 1, 1.0, 0.0)

    def row_bias(n, scales):
        total_bias = cb_ref[:, pl.ds(n, STEP)]
        if composed:
            for p in range(3):
                part = 0.0
                for q in range(3):
                    part += bias[3 * p + q, 0:1, pl.ds(n, STEP)] + bias[3 * p + q, 1:2, pl.ds(n, STEP)]
                total_bias = total_bias + part * scales[p]
        return total_bias

    def rows_at(a, n_rows):
        return pl.ds(pl.multiple_of(a * row_slots, 16), n_rows * row_slots)

    def conv(g, a, n_rows, first, final):
        @pl.loop(0, 1)
        def _(block_n):
            for part_n in range(width // STEP):
                n = part_n * STEP
                at_n = pl.ds(n, STEP)
                summed = None
                for p in range(3):
                    if composed:
                        chosen = pl.ds(pl.multiple_of((mine + g) % 2 * group_width, group_width), group_width)
                        weights = kernel_weights[p, :, chosen, at_n]
                    else:
                        weights = kernel_weights[p, :, :, at_n]
                    part = jnp.dot(
                        taps[g, rows_at(a + p, n_rows), :],
                        weights.reshape(3 * group_width, STEP),
                        preferred_element_type=jnp.float32,
                    )
                    summed = part if summed is None else summed + part
                if first:
                    shift = row_bias(n, (1.0, 1.0, 1.0))
                    above, below = row_bias(n, (top, 1.0, 1.0)), row_bias(n, (1.0, 1.0, bottom))
                for k in range(n_rows):
                    value = summed[k * row_slots : (k + 1) * row_slots]
                    if first:
                        value = value + (above if k == 0 else below if k == rows - 1 else shift)
                    else:
                        value = value + acc[rows_at(a + k, 1), at_n]
                    if final:
                        value = 0.5 * value * (1.0 + lax.erf(value * (0.5 ** 0.5)))
                        out_ref[a + k, :, at_n] = value[:cols].astype(jnp.bfloat16)
                    else:
                        acc[rows_at(a + k, 1), at_n] = value

    if composed:
        wait_edge(0)
        wait_near(0)
        wait_far(0)
        place_near(0)
        place_far(0)
        wait_rest(0)
        place_rest(0)
        conv(0, 0, rows, True, False)
        wait_near(1)
        wait_far(1)
        place_near(1)
        place_far(1)
        wait_rest(1)
        place_rest(1)
        conv(1, 0, rows, False, True)
    else:
        wait_edge(0)
        for other in range(2):
            wait_rest(other)
            wait_near(other)
            wait_far(other)
        place_rest(0)
        place_near(0)
        place_far(0)
        conv(0, 0, rows, True, True)

    sent = pl.ds(0, total - 1)
    arrived(recv.at[sent], send_sem)
    targets = (lat_n - 2) * lon_n

    @pl.when(inside)
    def _():
        arrived(recv_far.at[pl.ds(0, targets - 1)], fsend_sem)

    @pl.when(jnp.logical_not(inside))
    def _():
        arrived(recv_far.at[pl.ds(0, targets)], fsend_sem)

    arrived(near.at[pl.ds(0, count - 1)], nsend_sem.at[0])
    near_copy().wait_send()


def per_device(raw_fields, embed_weight, embed_bias, conv_weight, conv_bias):
    lat_n = lax.axis_size("lat")
    lon_n = lax.axis_size("lon")
    total = lat_n * lon_n
    var_dev, height, breadth = raw_fields.shape
    assert var_dev == 1 and lat_n % 4 == 0
    rows = height // lat_n // PATCH
    cols = breadth // lon_n // PATCH
    width = embed_weight.shape[3]
    row_slots = (cols + 2 + 15) // 16 * 16
    spare = LANES - row_slots
    assert LANES // 2 < row_slots < LANES and spare * (rows - 2) == row_slots
    assert row_slots - LANES // 2 <= spare
    dims = (lat_n, lon_n, height, breadth, rows, cols, width)
    group = min(lat_n, 8)
    bf16 = jnp.bfloat16
    composed = total * CELLS <= width
    tap_width = total * CELLS if composed else width
    groups = 2 if composed else 1
    any_space = pl.BlockSpec(memory_space=pltpu.HBM)
    vmem = pl.BlockSpec(memory_space=pltpu.VMEM)
    return pl.pallas_call(
        functools.partial(kernel, dims),
        out_shape=jax.ShapeDtypeStruct((rows, cols, width), bf16),
        in_specs=[any_space]*5,
        out_specs=vmem,
        scratch_shapes=[
            pltpu.VMEM((1, width), jnp.float32),
            pltpu.VMEM((1, width), jnp.float32),
            pltpu.VMEM((height, breadth), bf16),
            pltpu.VMEM((PATCH * group * rows * PATCH, lon_n * LANES), bf16),
            pltpu.VMEM((lat_n, lon_n, CELLS, (rows - 1) * LANES), bf16),
            pltpu.VMEM((lat_n, lon_n, CELLS // 2, LANES), bf16),
            pltpu.VMEM((lat_n, lon_n, CELLS, LANES), bf16),
            pltpu.VMEM((total, CELLS, (rows - 1) * LANES), bf16),
            pltpu.VMEM((total, CELLS // 2, LANES), bf16),
            pltpu.VMEM((total, CELLS, LANES), bf16),
            pltpu.VMEM((total, PATCH, PATCH, width), bf16),
            pltpu.VMEM((total + 1, CELLS, width), bf16),
            pltpu.VMEM((3, 3, width, width), bf16),
            pltpu.VMEM((3, 3, tap_width if composed else CELLS, width), bf16),
            pltpu.VMEM((9, 8, width), jnp.float32),
            pltpu.VMEM((groups, (rows + 2) * row_slots, 3 * tap_width // groups), bf16),
            pltpu.VMEM((rows * row_slots, width if composed else LANES), jnp.float32),
            pltpu.SemaphoreType.DMA,
            pltpu.SemaphoreType.DMA,
            pltpu.SemaphoreType.DMA,
            pltpu.SemaphoreType.DMA,
            pltpu.SemaphoreType.DMA((18,)),
            pltpu.SemaphoreType.DMA,
            pltpu.SemaphoreType.DMA,
            pltpu.SemaphoreType.DMA((2,)),
            pltpu.SemaphoreType.DMA((2,)),
            pltpu.SemaphoreType.DMA((2,)),
            pltpu.SemaphoreType.DMA((2,)),
            pltpu.SemaphoreType.DMA((2,)),
        ],
        compiler_params=pltpu.CompilerParams(
            collective_id=0, has_side_effects=True, vmem_limit_bytes=50 * 1024 * 1024
        ),
        name="tiles",
    )(
        *(pltpu.with_memory_space_constraint(v, pltpu.HBM) for v in (raw_fields, embed_weight, embed_bias.reshape(1, width), conv_weight, conv_bias.reshape(1, width))),
    )


def solution(mesh):
    return jax.shard_map(
        per_device,
        mesh=mesh,
        in_specs=(P(("lat", "lon"), None, None), P(), P(), P(), P()),
        out_specs=P("lat", "lon", None),
        check_vma=False,
    )
```

```python
import functools

import jax
import jax.numpy as jnp
from jax import lax
from jax.experimental import pallas as pl
from jax.experimental.pallas import tpu as pltpu
from jax.sharding import PartitionSpec as P

PATCH = 4
LANES = 128
CELLS = PATCH * PATCH
MESH = pl.DeviceIdType.MESH
STEP = 256
WINDOW = 9
FIRST = 6
FORWARD = (11, 14)


def kernel(
    dims,
    raw_hbm, ew_hbm, eb_hbm, cw_hbm, cb_hbm,
    out_ref,
    eb_ref, cb_ref, raw, sides, send, send_far, far_ends, recv, recv_far, near, ew_raw, ew, cw, comb, bias, taps, nine, acc,
    eb_sem, cb_sem, raw_sem, ew_sem, cw_sem, send_sem, fsend_sem, nsend_sem,
    edge_sem, rest_sem, far_sem, near_sem,
):
    lat_n, lon_n, height, breadth, rows, cols, width = dims
    total = lat_n * lon_n
    half_n = lat_n // 2
    lat = lax.axis_index("lat")
    lon = lax.axis_index("lon")
    me = lat * lon_n + lon
    mine = lat // half_n
    odd = lat % 2
    inside = (lat > 0) & (lat < lat_n - 1)
    row_slots = taps.shape[0] // (rows + 2)
    composed = total * CELLS <= width
    tap_width = total * CELLS if composed else width
    spare = LANES - row_slots
    tail = row_slots - LANES // 2
    tiles_n = rows - 1
    last = (tiles_n - 1) * LANES
    unrolled = total <= 32

    raw_copy = pltpu.make_async_copy(raw_hbm.at[0], raw, raw_sem)
    raw_copy.start()

    def peers(other, body):
        @pl.loop(1 - other, half_n * lon_n, unroll=unrolled)
        def _(step):
            k = step // lon_n
            base = (mine + other) % 2 * half_n
            local = k if other else (lat + k) % half_n
            body(base + local, (lon + step) % lon_n)

    barrier = pltpu.get_barrier_semaphore()

    def greet(a, b):
        pl.semaphore_signal(barrier, inc=1, device_id=(a, b), device_id_type=MESH)

    peers(1, greet)
    peers(0, greet)

    ew_copy = pltpu.make_async_copy(ew_hbm, ew_raw, ew_sem)
    ew_copy.start()
    bias_copies = [
        pltpu.make_async_copy(eb_hbm, eb_ref, eb_sem),
        pltpu.make_async_copy(cb_hbm, cb_ref, cb_sem),
    ]
    for copy in bias_copies:
        copy.start()

    unit_n = width // 2
    units = 18

    def fetch(unit):
        p, q, n = unit // 6, unit // 2 % 3, pl.multiple_of(unit % 2 * unit_n, unit_n)
        return pltpu.make_async_copy(
            cw_hbm.at[p, q, :, pl.ds(n, unit_n)], cw.at[p, q, :, pl.ds(n, unit_n)], cw_sem.at[unit]
        )

    patches = breadth // PATCH
    group = min(lat_n, 8)
    group_rows = group * rows * PATCH
    block = group * CELLS
    lane = lax.broadcasted_iota(jnp.int32, (1, PATCH * LANES), 1)
    slot = lane % LANES
    cell = lane // LANES
    m = lax.broadcasted_iota(jnp.int32, (rows * block, 1), 0)
    target = (
        (m % PATCH) * group_rows
        + ((m // CELLS) % group) * (rows * PATCH)
        + (m // block) * PATCH
        + (m // PATCH) % PATCH
    )
    c = lax.broadcasted_iota(jnp.int32, (rows * block, PATCH * group_rows), 1)
    pick_rows = jnp.where(c == target, 1.0, 0.0).astype(jnp.bfloat16)
    pickers = []
    for l in range(lon_n):
        wanted = [PATCH * ((cols * l - 1 + s) % patches) for s in range(cols + 2)]
        used = sorted({x // LANES for w in wanted for x in (w, w + PATCH - 1)})
        patch = (cols * l - 1 + slot + patches) % patches
        column = jnp.where(slot < cols + 2, PATCH * patch + cell, -1)
        picks = []
        for b in used:
            k = lax.broadcasted_iota(jnp.int32, (LANES, PATCH * LANES), 0) + b * LANES
            picks.append(jnp.where(k == column, 1.0, 0.0).astype(jnp.bfloat16))
        pickers.append((used, jnp.concatenate(picks, axis=0)))

    @pl.when(jnp.logical_not(inside))
    def _():
        recv_far[...] = jnp.zeros(recv_far.shape, jnp.bfloat16)

    for unit in range(FIRST):
        fetch(unit).start()
    raw_copy.wait()
    left_half = lax.broadcasted_iota(jnp.int32, (CELLS // 2, LANES), 1) < LANES // 2
    for g in range(lat_n // group):
        for l in range(lon_n):
            used, picks = pickers[l]
            parts = []
            for b in used:
                part = raw[
                    g * group_rows : (g + 1) * group_rows,
                    b * LANES : min((b + 1) * LANES, breadth),
                ]
                short = LANES - part.shape[1]
                if short:
                    fill = jnp.zeros((group_rows, short), jnp.bfloat16)
                    part = jnp.concatenate([part, fill], axis=1)
                parts.append(part)
            found = jnp.dot(
                jnp.concatenate(parts, axis=1), picks, preferred_element_type=jnp.float32
            ).astype(jnp.bfloat16)
            for j in range(PATCH):
                sides[j * group_rows : (j + 1) * group_rows, l * LANES : (l + 1) * LANES] = (
                    found[:, j * LANES : (j + 1) * LANES]
                )
        tiles = jnp.dot(pick_rows, sides[...], preferred_element_type=jnp.float32)
        low = lax.broadcasted_iota(jnp.int32, (block, LANES), 1) < row_slots
        even = lax.broadcasted_iota(jnp.int32, (block, LANES), 0) // CELLS % 2 == 0
        for l in range(lon_n):
            column = tiles[:, l * LANES : (l + 1) * LANES]
            per_row = [column[a * block : (a + 1) * block] for a in range(rows)]
            spread = per_row[rows - 2]
            here = slice(g * group, (g + 1) * group)
            turned = [pltpu.roll(spread, row_slots - k * spare, 1) for k in range(tiles_n - 1)]
            for k in range(tiles_n):
                kept = per_row[k if k < rows - 2 else rows - 1]
                kept = jnp.where(
                    low, kept, jnp.where(even, turned[min(k, tiles_n - 2)], turned[max(k - 1, 0)])
                )
                send[here, l, :, k * LANES : (k + 1) * LANES] = (
                    kept.astype(jnp.bfloat16).reshape(group, CELLS, LANES)
                )
            for t in range(group):
                at = g * group + t
                to = at + 1 if t % 2 else at - 1
                if 0 <= to < lat_n:
                    far = per_row[rows - 1 if t % 2 else 0][t * CELLS : (t + 1) * CELLS]
                    ends = pltpu.roll(far, spare, 1).astype(jnp.bfloat16)
                    far_ends[to, l, :, row_slots:] = ends[:, row_slots:]
                    folded = jnp.where(
                        left_half, far[: CELLS // 2], pltpu.roll(far[CELLS // 2 :], LANES // 2, 1)
                    )
                    send_far[to, l] = folded.astype(jnp.bfloat16)
                if at in (0, lat_n - 1):
                    far_ends[at, l, :, row_slots:] = jnp.zeros((CELLS, spare), jnp.bfloat16)
    for t in range(lat_n):
        tile = 0 if t % 2 else last
        send[t, :, :, tile + row_slots : tile + LANES] = far_ends[t, :, :, row_slots:]

    for unit in range(FIRST, WINDOW):
        fetch(unit).start()

    ew_copy.wait()
    for copy in bias_copies:
        copy.wait()
    for i in range(PATCH):
        ew[:total, PATCH * i : PATCH * (i + 1), :] = ew_raw[:, i]
    if composed:
        high = eb_ref[...].astype(jnp.bfloat16)
        rest = eb_ref[...] - high.astype(jnp.float32)
        index = lax.broadcasted_iota(jnp.int32, (CELLS, width), 0)
        both = jnp.where(index == 0, high.astype(jnp.float32), jnp.where(index == 1, rest, 0.0))
        ew[total] = both.astype(jnp.bfloat16)

    def compose(start, stop):
        for unit in range(start, stop):
            fetch(unit).wait()
        for unit in range(start + WINDOW, min(stop + WINDOW, units)):
            fetch(unit).start()
        if composed:
            left = ew[...].reshape((total + 1) * CELLS, width)
            for unit in range(start, stop):
                p, q = unit // 6, unit // 2 % 3
                for step in range(0, unit_n, STEP):
                    n = unit % 2 * unit_n + step
                    product = jnp.dot(
                        left, cw[p, q, :, n : n + STEP], preferred_element_type=jnp.float32
                    )
                    comb[p, q, :, n : n + STEP] = product[:tap_width].astype(jnp.bfloat16)
                    bias[3 * p + q, :, n : n + STEP] = product[tap_width : tap_width + 8]

    def edge_tile(parity):
        return pl.multiple_of((1 - parity) * last, LANES)

    def rest_tiles(parity):
        return pl.multiple_of(parity * LANES, LANES)

    def remote(source, dest, out_sem, in_sem, a, b):
        pltpu.make_async_remote_copy(
            src_ref=source, dst_ref=dest, send_sem=out_sem, recv_sem=in_sem,
            device_id=(a, b), device_id_type=MESH,
        ).start()

    quarter_n = lat_n // 4
    quarter = lat // quarter_n

    def relation(a):
        there = a // quarter_n
        return (there // 2 + quarter // 2) % 2 * 2 + (there + quarter) % 2

    def exchange(part, other):
        def body(a, b):
            if part == "edge":
                at = pl.ds(edge_tile(a % 2), LANES)
                remote(send.at[a, b, :, at], recv.at[me, :, at], send_sem, edge_sem.at[other], a, b)
            if part == "near":
                at = pl.ds(edge_tile(1 - a % 2), LANES)
                source = send.at[a + 1 - 2 * (a % 2), b, :, at]
                remote(source, near.at[me], nsend_sem.at[0], near_sem.at[0], a, b)
            if part == "rest":
                at = pl.ds(rest_tiles(a % 2), last)
                remote(send.at[a, b, :, at], recv.at[me, :, at], send_sem, rest_sem.at[relation(a)], a, b)
            if part == "far":
                @pl.when((a > 0) & (a < lat_n - 1))
                def _():
                    remote(send_far.at[a, b], recv_far.at[me], fsend_sem, far_sem.at[other], a, b)

        peers(other, body)

    def issue():
        pl.semaphore_wait(barrier, total - 1)
        exchange("edge", 1)
        exchange("edge", 0)
        exchange("near", 0)
        exchange("far", 0)
        exchange("far", 1)
        exchange("rest", 0)
        exchange("rest", 1)
        own = pl.ds(edge_tile(odd), LANES)
        pltpu.make_async_copy(send.at[lat, lon, :, own], recv.at[me, :, own], edge_sem.at[0]).start()
        pair = pl.ds(edge_tile(1 - odd), LANES)
        pltpu.make_async_copy(
            send.at[lat + 1 - 2 * odd, lon, :, pair], near.at[me], near_sem.at[0]
        ).start()
        own = pl.ds(rest_tiles(odd), last)
        pltpu.make_async_copy(send.at[lat, lon, :, own], recv.at[me, :, own], rest_sem.at[0]).start()

        @pl.when(inside)
        def _():
            pltpu.make_async_copy(send_far.at[lat, lon], recv_far.at[me], far_sem.at[0]).start()

    count = half_n * lon_n

    def sources(other):
        return pl.ds(pl.multiple_of((mine + other) % 2 * count, count), count)

    def near_copy():
        return pltpu.make_async_remote_copy(
            src_ref=recv.at[sources(1), :, pl.ds(edge_tile(odd), LANES)],
            dst_ref=near.at[sources(1)],
            send_sem=nsend_sem.at[1],
            recv_sem=near_sem.at[1],
            device_id=(lat + 1 - 2 * odd, lon),
            device_id_type=MESH,
        )

    def arrived(ref, sem):
        pltpu.make_async_copy(ref, ref, sem).wait()

    def wait_edge(other):
        arrived(recv.at[sources(other), :, pl.ds(0, LANES)], edge_sem.at[other])

    def forward_near():
        wait_edge(1)
        near_copy().start()

    def wait_near(other):
        arrived(near.at[sources(other)], near_sem.at[other])

    def wait_rest(rel):
        arrived(recv.at[pl.ds(0, count // 2), :, pl.ds(0, last)], rest_sem.at[rel])

    def wait_far(other):
        @pl.when(inside)
        def _():
            arrived(recv_far.at[sources(other)], far_sem.at[other])

    hops = lat // 2 + odd + lon // 2
    early = (0, 1, 3, 6)
    for k, stop in enumerate(early):
        if k:
            compose(early[k - 1], stop)
        pl.when(jnp.maximum(len(early) - 1 - hops, 0) == k)(issue)
    compose(early[-1], FORWARD[0])
    pl.when(hops > 0)(forward_near)
    compose(FORWARD[0], FORWARD[1])
    pl.when(hops == 0)(forward_near)
    compose(FORWARD[1], units)

    group_width = tap_width // 2 if composed else tap_width
    quarter_width = tap_width // 4
    middle = jnp.where(quarter < lat_n // quarter_n - 1, 2, 3)
    stages = ((0,), (1, middle), (5 - middle,))

    def quarter_of(rel):
        return (quarter // 2 + rel // 2) % 2 * 2 + (quarter + rel) % 2

    def part_of(rel, size):
        return pl.ds(pl.multiple_of(quarter_of(rel) * size, size), size)

    def taken(ref, g, at=slice(None)):
        if not composed:
            return ref[:, :, at]
        return jnp.concatenate(
            [ref[part_of(rel, count // 2), :, at] for rel in stages[g]], axis=0
        )

    def place(g, row, n, tokens):
        for q in range(3):
            shifted = tokens if q == 0 else pltpu.roll(tokens, row_slots - q, 0)
            shifted = shifted.astype(jnp.bfloat16)
            if g == 1 or not composed:
                start = row * row_slots
                if not isinstance(start, int):
                    start = pl.multiple_of(start, 16)
                lo = q * group_width + n
                taps[pl.ds(start, row_slots), lo : lo + tokens.shape[1]] = shifted
                continue
            if isinstance(row, int):
                targets = [(row - p, p) for p in range(3) if 0 <= row - p < rows]
            else:
                below = row // (rows + 1)
                targets = [((rows - 1) * below, 2 * below)]
            for at_row, p in targets:
                start = at_row * row_slots
                lo = (3 * p + q) * quarter_width
                if not isinstance(row, int):
                    start, lo = pl.multiple_of(start, 16), pl.multiple_of(lo, LANES)
                nine[g // 2, pl.ds(start, row_slots), pl.ds(lo, quarter_width)] = shifted

    def embed(x, n):
        if composed:
            return x.astype(jnp.float32)
        weights = ew[:total, :, n : n + STEP].reshape(total * CELLS, STEP)
        return jnp.dot(x, weights, preferred_element_type=jnp.float32) + eb_ref[:, n : n + STEP]

    def spans(g):
        return (0,) if composed else range(0, group_width, STEP)

    def flat(x):
        return x.reshape(x.shape[0] * CELLS, x.shape[2]).T

    def place_rest(g):
        x = flat(taken(recv, g))
        for n in spans(g):
            e = embed(x, n)
            chunks = []
            for k in range(tiles_n):
                row = k if k < rows - 2 else rows - 1
                place(g, row + 1, n, e[k * LANES : k * LANES + row_slots])
                chunks.append(e[k * LANES + row_slots : (k + 1) * LANES])
            kept = [
                jnp.where(odd > 0, chunks[k + 1], chunks[k]) for k in range(tiles_n - 1)
            ]
            place(g, rows - 1, n, jnp.concatenate(kept, axis=0)[:row_slots])

    def place_near(g):
        x = flat(taken(near, g))[:row_slots]
        for n in spans(g):
            place(g, (rows + 1) * (1 - odd), n, embed(x, n))

    def place_far(g):
        folded = taken(recv_far, g).astype(jnp.float32)
        n_src = folded.shape[0]
        turned = pltpu.roll(folded.reshape(n_src * CELLS // 2, LANES), LANES // 2, 1)
        whole = jnp.concatenate([folded, turned.reshape(folded.shape)], axis=1)
        x = flat(whole)[: LANES // 2].astype(jnp.bfloat16)
        at = pl.ds(edge_tile(odd), LANES)
        edge = taken(recv, g, at)
        ends = flat(edge)[row_slots : row_slots + tail]
        x = jnp.concatenate([x, ends], axis=0)
        for n in spans(g):
            e = embed(x, n)
            if not composed:
                e = e * jnp.where(inside, 1.0, 0.0)
            place(g, (rows + 1) * odd, n, e)

    top = jnp.where(lat > 0, 1.0, 0.0)
    bottom = jnp.where(lat < lat_n - 1, 1.0, 0.0)

    def row_bias(n, scales):
        total_bias = cb_ref[:, pl.ds(n, STEP)]
        if composed:
            for p in range(3):
                part = 0.0
                for q in range(3):
                    part += bias[3 * p + q, 0:1, pl.ds(n, STEP)] + bias[3 * p + q, 1:2, pl.ds(n, STEP)]
                total_bias = total_bias + part * scales[p]
        return total_bias

    def rows_at(a, n_rows):
        return pl.ds(pl.multiple_of(a * row_slots, 16), n_rows * row_slots)

    def conv(g, a, n_rows, first, final):
        @pl.loop(0, 1)
        def _(block_n):
            for part_n in range(width // STEP):
                n = part_n * STEP
                at_n = pl.ds(n, STEP)
                if composed and g != 1:
                    weights = comb[:, :, part_of(stages[g][0], quarter_width), at_n]
                    summed = jnp.dot(
                        nine[g // 2], weights.reshape(9 * quarter_width, STEP),
                        preferred_element_type=jnp.float32,
                    )
                else:
                    summed = None
                    for p in range(3):
                        if composed:
                            weights = jnp.concatenate(
                                [comb[p, :, part_of(rel, quarter_width), at_n] for rel in stages[g]],
                                axis=1,
                            )
                        else:
                            weights = cw[p, :, :, at_n]
                        part = jnp.dot(
                            taps[rows_at(a + p, n_rows), :],
                            weights.reshape(3 * group_width, STEP),
                            preferred_element_type=jnp.float32,
                        )
                        summed = part if summed is None else summed + part
                if first:
                    shift = row_bias(n, (1.0, 1.0, 1.0))
                    above, below = row_bias(n, (top, 1.0, 1.0)), row_bias(n, (1.0, 1.0, bottom))
                for k in range(n_rows):
                    value = summed[k * row_slots : (k + 1) * row_slots]
                    if first:
                        value = value + (above if k == 0 else below if k == rows - 1 else shift)
                    else:
                        value = value + acc[rows_at(a + k, 1), at_n]
                    if final:
                        value = 0.5 * value * (1.0 + lax.erf(value * (0.5 ** 0.5)))
                        out_ref[a + k, :, at_n] = value[:cols].astype(jnp.bfloat16)
                    else:
                        acc[rows_at(a + k, 1), at_n] = value

    wait_edge(0)
    if composed:
        wait_near(0)
        wait_far(0)
        wait_rest(0)
        place_rest(0)
        place_near(0)
        place_far(0)
        conv(0, 0, rows, True, False)
        wait_near(1)
        wait_far(1)
        place_near(1)
        place_far(1)
        wait_rest(1)
        wait_rest(middle)
        place_rest(1)
        conv(1, 0, rows, False, False)
        place_near(2)
        place_far(2)
        wait_rest(5 - middle)
        place_rest(2)
        conv(2, 0, rows, False, True)
    else:
        for rel in range(4):
            wait_rest(rel)
        for other in range(2):
            wait_near(other)
            wait_far(other)
        place_rest(0)
        place_near(0)
        place_far(0)
        conv(0, 0, rows, True, True)

    sent = pl.ds(0, total - 1)
    arrived(recv.at[sent], send_sem)
    targets = (lat_n - 2) * lon_n

    @pl.when(inside)
    def _():
        arrived(recv_far.at[pl.ds(0, targets - 1)], fsend_sem)

    @pl.when(jnp.logical_not(inside))
    def _():
        arrived(recv_far.at[pl.ds(0, targets)], fsend_sem)

    arrived(near.at[pl.ds(0, count - 1)], nsend_sem.at[0])
    near_copy().wait_send()


def per_device(raw_fields, embed_weight, embed_bias, conv_weight, conv_bias):
    lat_n = lax.axis_size("lat")
    lon_n = lax.axis_size("lon")
    total = lat_n * lon_n
    var_dev, height, breadth = raw_fields.shape
    assert var_dev == 1 and lat_n % 4 == 0
    rows = height // lat_n // PATCH
    cols = breadth // lon_n // PATCH
    width = embed_weight.shape[3]
    row_slots = (cols + 2 + 15) // 16 * 16
    spare = LANES - row_slots
    assert LANES // 2 < row_slots < LANES and spare * (rows - 2) == row_slots
    assert row_slots - LANES // 2 <= spare
    dims = (lat_n, lon_n, height, breadth, rows, cols, width)
    group = min(lat_n, 8)
    bf16 = jnp.bfloat16
    composed = total * CELLS <= width
    tap_width = total * CELLS if composed else width
    any_space = pl.BlockSpec(memory_space=pltpu.HBM)
    vmem = pl.BlockSpec(memory_space=pltpu.VMEM)
    return pl.pallas_call(
        functools.partial(kernel, dims),
        out_shape=jax.ShapeDtypeStruct((rows, cols, width), bf16),
        in_specs=[any_space]*5,
        out_specs=vmem,
        scratch_shapes=[
            pltpu.VMEM((1, width), jnp.float32),
            pltpu.VMEM((1, width), jnp.float32),
            pltpu.VMEM((height, breadth), bf16),
            pltpu.VMEM((PATCH * group * rows * PATCH, lon_n * LANES), bf16),
            pltpu.VMEM((lat_n, lon_n, CELLS, (rows - 1) * LANES), bf16),
            pltpu.VMEM((lat_n, lon_n, CELLS // 2, LANES), bf16),
            pltpu.VMEM((lat_n, lon_n, CELLS, LANES), bf16),
            pltpu.VMEM((total, CELLS, (rows - 1) * LANES), bf16),
            pltpu.VMEM((total, CELLS // 2, LANES), bf16),
            pltpu.VMEM((total, CELLS, LANES), bf16),
            pltpu.VMEM((total, PATCH, PATCH, width), bf16),
            pltpu.VMEM((total + 1, CELLS, width), bf16),
            pltpu.VMEM((3, 3, width, width), bf16),
            pltpu.VMEM((3, 3, tap_width if composed else CELLS, width), bf16),
            pltpu.VMEM((9, 8, width), jnp.float32),
            pltpu.VMEM(((rows + 2) * row_slots, 3 * tap_width // (2 if composed else 1)), bf16),
            pltpu.VMEM((2, rows * row_slots if composed else CELLS, 9 * tap_width // 4), bf16),
            pltpu.VMEM((rows * row_slots, width if composed else LANES), jnp.float32),
            pltpu.SemaphoreType.DMA,
            pltpu.SemaphoreType.DMA,
            pltpu.SemaphoreType.DMA,
            pltpu.SemaphoreType.DMA,
            pltpu.SemaphoreType.DMA((18,)),
            pltpu.SemaphoreType.DMA,
            pltpu.SemaphoreType.DMA,
            pltpu.SemaphoreType.DMA((2,)),
            pltpu.SemaphoreType.DMA((2,)),
            pltpu.SemaphoreType.DMA((4,)),
            pltpu.SemaphoreType.DMA((2,)),
            pltpu.SemaphoreType.DMA((2,)),
        ],
        compiler_params=pltpu.CompilerParams(
            collective_id=0, has_side_effects=True, vmem_limit_bytes=50 * 1024 * 1024
        ),
        name="tiles",
    )(
        *(pltpu.with_memory_space_constraint(v, pltpu.HBM) for v in (raw_fields, embed_weight, embed_bias.reshape(1, width), conv_weight, conv_bias.reshape(1, width))),
    )


def solution(mesh):
    return jax.shard_map(
        per_device,
        mesh=mesh,
        in_specs=(P(("lat", "lon"), None, None), P(), P(), P(), P()),
        out_specs=P("lat", "lon", None),
        check_vma=False,
    )
```
